32 devices in a mesh: dp: 4 (over x, y), tp: 8 (over z, core).
Axes of the slice: x: 2, y: 2, z: 4, core: 2. Of those that a mesh axis runs over, the one named last changes fastest.
Arguments:
- x: bfloat16 [256, 3072], P('dp'), parts along dimension 0
- k_cache: bfloat16 [256, 4096, 8, 128], P('dp', None, 'tp'), parts along dimension 0
- v_cache: bfloat16 [256, 4096, 8, 128], P('dp', None, 'tp'), parts along dimension 0
- gain_a: bfloat16 [3072], replicated
- wq: bfloat16 [3072, 3072], P(None, 'tp')
- wo: bfloat16 [3072, 3072], P('tp')
- gain_m: bfloat16 [3072], replicated
- w_gate: bfloat16 [3072, 8192], P(None, 'tp')
- w_up: bfloat16 [3072, 8192], P(None, 'tp')
- w_down: bfloat16 [8192, 3072], P('tp')
Outputs:
- output: bfloat16 [256, 3072], P('dp'), parts along dimension 0
There are 4 independent parts. The reference program is written for one: setup_inputs(seed, part) draws one part's arguments, and reference() takes and returns one part's arrays. A program takes and returns all parts, laid end to end along the dimension named above; an argument that names none is the same for every part.
All inputs are finite; a program needn't handle non-finite values.
Results may differ from the reference program's by a relative error of at most 0.017.
Values are sent between devices in bfloat16 or wider.
A program may use at most 2 GiB of HBM per device.

```python
import jax
import jax.numpy as jnp
from jax import lax

BATCH = 64
CACHE = 4096
D = 3072
HEADS = 24
KV_HEADS = 8
HEAD = 128
FF = 8192
THETA = 10000


def setup_inputs(seed: int = 0, part: int = 0) -> dict:
    kx, kc, kw, kn, kq, ko, km, kg, ku, kd = jax.random.split(jax.random.key(seed), 10)
    kx, kc, kw = (jax.random.fold_in(k, part) for k in (kx, kc, kw))

    def weights(key, rows, columns):
        return jax.random.normal(key, (rows, columns), jnp.float32) * rows**-0.5

    drawn = {
        "x": jax.random.normal(kx, (BATCH, D), jnp.float32),
        "k_cache": 2 * jax.random.normal(kc, (BATCH, CACHE, KV_HEADS, HEAD), jnp.float32),
        "v_cache": 4 * jax.random.normal(kw, (BATCH, CACHE, KV_HEADS, HEAD), jnp.float32),
        "gain_a": 1 + 0.1 * jax.random.normal(kn, (D,), jnp.float32),
        "wq": 2 * weights(kq, D, HEADS * HEAD),
        "wo": weights(ko, HEADS * HEAD, D),
        "gain_m": 1 + 0.1 * jax.random.normal(km, (D,), jnp.float32),
        "w_gate": weights(kg, D, FF),
        "w_up": weights(ku, D, FF),
        "w_down": 2 * weights(kd, FF, D),
    }
    return {k: v.astype(jnp.bfloat16) for k, v in drawn.items()}


def normed(x, gain):
    wide = x.astype(jnp.float32)
    scale = lax.rsqrt(jnp.mean(wide * wide, -1, keepdims=True) + 1e-6)
    return (wide * scale * gain.astype(jnp.float32)).astype(jnp.bfloat16)


def turned(t, place, theta):
    half = t.shape[-1] // 2
    angle = place.astype(jnp.float32)[:, None] * theta ** (-jnp.arange(half, dtype=jnp.float32) / half)
    cos, sin = jnp.cos(angle)[:, None], jnp.sin(angle)[:, None]
    a, b = t[..., :half].astype(jnp.float32), t[..., half:].astype(jnp.float32)
    return jnp.concatenate([a * cos - b * sin, b * cos + a * sin], -1).astype(jnp.bfloat16)


def matmul(a, w):
    return jnp.dot(a, w, preferred_element_type=jnp.float32).astype(jnp.bfloat16)


def einsum(form, a, b):
    return jnp.einsum(form, a.astype(jnp.float32), b.astype(jnp.float32))


def seen_by(a, wq, k_cache, v_cache, head, theta):
    batch, cache, kv_heads = k_cache.shape[:3]
    place = jnp.full((batch,), cache - 1)
    q = turned(matmul(a, wq).reshape(batch, -1, head), place, theta).reshape(batch, kv_heads, -1, head)
    scores = einsum("bgsd,bugd->bgsu", q, k_cache) * head**-0.5
    weights = jax.nn.softmax(scores, -1).astype(jnp.bfloat16)
    return einsum("bgsu,bugd->bgsd", weights, v_cache).astype(jnp.bfloat16).reshape(batch, -1)


def hidden_of(b, w_gate, w_up):
    gate = jnp.dot(b, w_gate, preferred_element_type=jnp.float32)
    up = jnp.dot(b, w_up, preferred_element_type=jnp.float32)
    return (jax.nn.silu(gate) * up).astype(jnp.bfloat16)


def reference(x, k_cache, v_cache, gain_a, wq, wo, gain_m, w_gate, w_up, w_down):
    seen = seen_by(normed(x, gain_a), wq, k_cache, v_cache, HEAD, THETA)
    h = (x.astype(jnp.float32) + jnp.dot(seen, wo, preferred_element_type=jnp.float32)).astype(jnp.bfloat16)
    hidden = hidden_of(normed(h, gain_m), w_gate, w_up)
    return (h.astype(jnp.float32) + jnp.dot(hidden, w_down, preferred_element_type=jnp.float32)).astype(jnp.bfloat16)
```

```python
import functools

import jax
import jax.numpy as jnp
import numpy as np
from jax import lax
from jax.experimental import pallas as pl
from jax.experimental.pallas import tpu as pltpu
from jax.sharding import PartitionSpec as P

HEAD = 128
THETA = 10000
SEQS, CACHE, D, FF, TP = 64, 4096, 3072, 8192, 8
QH = 3
HALF = D // 2
HID = FF // TP
SLOTS = 6
UNIT = 2
STEPS = SEQS // (2 * UNIT)
F32, BF16 = jnp.float32, jnp.bfloat16

GROUPS = (24, 16, 16, 8)
AFTER = {
    5: [("wo", 0)],
    6: [("share1", 0)],
    9: [("wo", 1)],
    10: [("share1", 1), ("h", 0)],
    11: [("mlp", 0)],
    12: [("share2", 0)],
    13: [("wo", 2)],
    14: [("share1", 2), ("h", 1)],
    15: [
        ("wo", 3), ("share1", 3), ("mlp", 1), ("share2", 1), ("y", 0), ("h", 2), ("mlp", 2), ("share2", 2), ("h", 3), ("mlp", 3),
        ("share2", 3), ("out", 0), ("y", 1), ("out", 1), ("y", 2), ("out", 2), ("y", 3), ("out", 3),
    ],
}


def rotary():
    half = HEAD // 2
    angle = np.float32(CACHE - 1) * np.float32(THETA) ** (-np.arange(half, dtype=np.float32) / np.float32(half))
    cos, sin = np.cos(angle), np.sin(angle)
    return np.concatenate([cos, cos]).astype(np.float32), np.concatenate([-sin, sin]).astype(np.float32)


def kernel(
    x_hbm, k_hbm, v_hbm, small_hbm, wq_hbm, wo_hbm, wg_hbm, wu_hbm, wd_hbm, y_hbm,
    small, wq, wo, wg, wu, wd, kbuf, vbuf, sbuf, obuf, qbuf, xs, sends, gots, mines, parts, halves,
    ksem, vsem, wsem, xsem, ysem, ssem, rsem,
):
    me = lax.axis_index("tp")
    z, c = me // 2, me % 2
    firsts = [sum(GROUPS[:g]) for g in range(len(GROUPS))]

    barrier = pltpu.get_barrier_semaphore()
    partner = 2 * z + (1 - c)
    others = [2 * lax.rem(z + d, 4) + c for d in (1, 2, 3)]
    for peer in (partner, *others):
        pl.semaphore_signal(barrier, inc=1, device_id={"tp": peer}, device_id_type=pl.DeviceIdType.MESH)

    xcopies = [
        pltpu.make_async_copy(x_hbm.at[pl.ds(firsts[g], rows), pl.ds(i * HALF, HALF)], xs[g].at[i], xsem.at[g, i])
        for g, rows in enumerate(GROUPS)
        for i in range(2)
    ]
    small_copy = pltpu.make_async_copy(small_hbm, small, wsem.at[0])
    wcopies = [
        pltpu.make_async_copy(source, target, wsem.at[1 + i])
        for i, (source, target) in enumerate([(wq_hbm, wq), (wo_hbm, wo), (wg_hbm, wg), (wu_hbm, wu), (wd_hbm, wd)])
    ]

    def kcopy(p):
        slot = lax.rem(p, SLOTS)
        return pltpu.make_async_copy(k_hbm.at[pl.ds(2 * p, 2)], kbuf.at[slot], ksem.at[slot])

    def vcopy(p):
        slot = lax.rem(p, SLOTS)
        return pltpu.make_async_copy(v_hbm.at[pl.ds(2 * p, 2)], vbuf.at[slot], vsem.at[slot])

    for copy in (*xcopies, small_copy, wcopies[0]):
        copy.start()
    for p in range(SLOTS):
        kcopy(p).start()
        vcopy(p).start()
    for copy in wcopies[1:]:
        copy.start()

    def normed(wide, gain):
        scale = lax.rsqrt(jnp.mean(wide * wide, -1, keepdims=True) + 1e-6)
        return (wide * scale * gain).astype(BF16)

    for copy in (*xcopies, small_copy, wcopies[0]):
        copy.wait()
    wide = jnp.concatenate([jnp.concatenate([x[0].astype(F32), x[1].astype(F32)], 1) for x in xs], 0)
    q = jnp.dot(normed(wide, small[0:1, :]), wq[...], preferred_element_type=F32).astype(BF16).astype(F32)
    cos, sin = small[2:3, 0:HEAD], small[3:4, 0:HEAD]
    qbuf[...] = jnp.zeros_like(qbuf)
    for s in range(QH):
        t = q[:, s * HEAD : (s + 1) * HEAD]
        turned = t * cos + pltpu.roll(t, HEAD // 2, 1) * sin
        qbuf[:, s, :] = turned.astype(BF16).astype(F32)

    tile = 256

    def scores(p):
        slot, kept = lax.rem(p, SLOTS), lax.rem(p, 2 * UNIT)
        first = qbuf[2 * p]
        second = pltpu.roll(qbuf[2 * p + 1], QH, 0)
        row = lax.broadcasted_iota(jnp.int32, first.shape, 0)
        second = jnp.where((row >= QH) & (row < 2 * QH), second, 0.0)
        both = jnp.concatenate([first, second], 1).astype(BF16)
        for i in range(CACHE // tile):
            at = pl.ds(i * tile, tile)
            keys = jnp.concatenate([kbuf[slot, 0, at, :], kbuf[slot, 1, at, :]], 1)
            found = lax.dot_general(both, keys, (((1,), (1,)), ((), ())), preferred_element_type=F32)
            sbuf[kept, :, at] = found * HEAD**-0.5

    def finish(p):
        slot, kept = lax.rem(p, SLOTS), lax.rem(p, 2 * UNIT)
        s = sbuf[kept]
        e = jnp.exp(s - jnp.max(s, -1, keepdims=True))
        w = (e * (1.0 / jnp.sum(e, -1, keepdims=True))).astype(BF16)
        sums = [None, None]
        for i in range(CACHE // tile):
            at = pl.ds(i * tile, tile)
            values = jnp.concatenate([vbuf[slot, 0, at, :], vbuf[slot, 1, at, :]], 1)
            term = jnp.dot(w[:, i * tile : (i + 1) * tile], values, preferred_element_type=F32)
            sums[i % 2] = term if sums[i % 2] is None else sums[i % 2] + term
        for i, total in enumerate(sums):
            obuf[i, pl.ds(pl.multiple_of(16 * p, 16), 8), :] = total[:, :HEAD]
            obuf[i, pl.ds(pl.multiple_of(16 * p + 8, 8), 8), :] = pltpu.roll(total[:, HEAD:], 8 - QH, 0)

    def step(k, last):
        for u in range(UNIT):
            vcopy(k * UNIT + u).wait()
            if not last:
                kcopy((k + 1) * UNIT + u).wait()
        for u in range(UNIT):
            finish(k * UNIT + u)
        if last:
            return
        for u in range(UNIT):
            scores((k + 1) * UNIT + u)
        for u in range(UNIT):
            for copy, p in ((vcopy, k * UNIT + u), (kcopy, (k + 1) * UNIT + u)):

                @pl.when(p + SLOTS < SEQS // 2)
                def _():
                    copy(p + SLOTS).start()

    def remote(n, g, i, source, target, peer):
        return pltpu.make_async_remote_copy(
            src_ref=source,
            dst_ref=target,
            send_sem=ssem.at[n, g, i],
            recv_sem=rsem.at[n, g, i],
            device_id={"tp": peer},
            device_id_type=pl.DeviceIdType.MESH,
        )

    def to_partner(n, g):
        return remote(n, g, 0, sends[n][g], gots[n][g], partner)

    def to_others(n, g):
        return [remote(n, g, d, parts[n][g].at[0], parts[n][g].at[d], others[d - 1]) for d in (1, 2, 3)]

    def halves_to_partner(n, g):
        return remote(n, g, 4, halves[n][g].at[c], halves[n][g].at[c], partner)

    def terms(n, g, left, right_ref):
        width = 512
        for mine in (False, True):
            base = (c if mine else 1 - c) * HALF
            for j in range(HALF // width):
                at = pl.ds(pl.multiple_of(base + j * width, width), width)
                term = jnp.dot(left, right_ref[:, at], preferred_element_type=F32)
                if mine:
                    mines[n][g][:, j * width : (j + 1) * width] = term
                else:
                    sends[n][g][:, j * width : (j + 1) * width] = term.astype(BF16)
            if not mine:
                to_partner(n, g).start()

    def share(n, g):
        to_partner(n, g).wait()
        parts[n][g][0] = (mines[n][g][...] + gots[n][g][...].astype(F32)).astype(BF16)
        for copy in to_others(n, g):
            copy.start()

    def summed(n, g, base):
        for copy in to_others(n, g):
            copy.wait()
        total = None
        for chip in range(4):
            part = parts[n][g][lax.rem(z - chip + 4, 4)].astype(F32)
            total = part if total is None else total + part
        halves[n][g][c] = (base.astype(F32) + total).astype(BF16)
        halves_to_partner(n, g).start()

    started = set()

    def do(what, g):
        rows = GROUPS[g]
        if what == "wo":
            if not started:
                pl.semaphore_wait(barrier, 4)
                wcopies[1].wait()
            started.add("wo")
            seen = []
            for s in range(QH):
                at = pl.ds(8 * firsts[g] + s, rows, stride=8)
                seen.append(obuf[0, at, :] + obuf[1, at, :])
            terms(0, g, jnp.concatenate(seen, 1).astype(BF16), wo)
        elif what == "share1":
            share(0, g)
        elif what == "h":
            summed(0, g, xs[g][c])
        elif what == "mlp":
            if "mlp" not in started:
                for copy in wcopies[2:]:
                    copy.wait()
            started.add("mlp")
            halves_to_partner(0, g).wait()
            h = jnp.concatenate([halves[0][g][0].astype(F32), halves[0][g][1].astype(F32)], 1)
            b = normed(h, small[1:2, :])
            hidden = []
            for j in range(HID // tile):
                at = pl.ds(j * tile, tile)
                gate = jnp.dot(b, wg[:, at], preferred_element_type=F32)
                up = jnp.dot(b, wu[:, at], preferred_element_type=F32)
                hidden.append((jax.nn.silu(gate) * up).astype(BF16))
            terms(1, g, jnp.concatenate(hidden, 1), wd)
        elif what == "share2":
            share(1, g)
        elif what == "y":
            summed(1, g, halves[0][g][c])
        elif what == "out":
            halves_to_partner(1, g).wait()
            for i in range(2):
                ycopy(g, i).start()

    def ycopy(g, i):
        return pltpu.make_async_copy(halves[1][g].at[i], y_hbm.at[pl.ds(firsts[g], GROUPS[g]), pl.ds(i * HALF, HALF)], ysem.at[g, i])

    for u in range(UNIT):
        kcopy(u).wait()
        scores(u)
        kcopy(u + SLOTS).start()
    at = 0
    for k in sorted(AFTER):
        if k < STEPS - 1:
            lax.fori_loop(at, k + 1, lambda i, _: step(i, False), None)
        else:
            if at < STEPS - 1:
                lax.fori_loop(at, STEPS - 1, lambda i, _: step(i, False), None)
            step(STEPS - 1, True)
        at = k + 1
        for what, g in AFTER[k]:
            do(what, g)
    for g in range(len(GROUPS)):
        for i in range(2):
            ycopy(g, i).wait()


def layer(x, k, v, small, wq, wo, wg, wu, wd):
    n = len(GROUPS)
    per_group = lambda *shape, dtype=BF16, lead=(): [pltpu.VMEM((*lead, rows, *shape), dtype) for rows in GROUPS]
    return pl.pallas_call(
        kernel,
        out_shape=jax.ShapeDtypeStruct((SEQS, D), BF16),
        in_specs=[pl.BlockSpec(memory_space=pltpu.HBM)] * 9,
        out_specs=pl.BlockSpec(memory_space=pltpu.HBM),
        scratch_shapes=[
            pltpu.VMEM(small.shape, F32),
            pltpu.VMEM(wq.shape, BF16),
            pltpu.VMEM(wo.shape, BF16),
            pltpu.VMEM(wg.shape, BF16),
            pltpu.VMEM(wu.shape, BF16),
            pltpu.VMEM(wd.shape, BF16),
            pltpu.VMEM((SLOTS, 2, CACHE, HEAD), BF16),
            pltpu.VMEM((SLOTS, 2, CACHE, HEAD), BF16),
            pltpu.VMEM((2 * UNIT, 8, CACHE), F32),
            pltpu.VMEM((2, SEQS * 8, HEAD), F32),
            pltpu.VMEM((SEQS, 8, HEAD), F32),
            per_group(HALF, lead=(2,)),
            [per_group(HALF), per_group(HALF)],
            [per_group(HALF), per_group(HALF)],
            [per_group(HALF, dtype=F32), per_group(HALF, dtype=F32)],
            [per_group(HALF, lead=(4,)), per_group(HALF, lead=(4,))],
            [per_group(HALF, lead=(2,)), per_group(HALF, lead=(2,))],
            pltpu.SemaphoreType.DMA((SLOTS,)),
            pltpu.SemaphoreType.DMA((SLOTS,)),
            pltpu.SemaphoreType.DMA((6,)),
            pltpu.SemaphoreType.DMA((n, 2)),
            pltpu.SemaphoreType.DMA((n, 2)),
            pltpu.SemaphoreType.DMA((2, n, 5)),
            pltpu.SemaphoreType.DMA((2, n, 5)),
        ],
        compiler_params=pltpu.CompilerParams(collective_id=0, has_side_effects=True, vmem_limit_bytes=63 * 2**20),
    )(x, k, v, small, wq, wo, wg, wu, wd)


def solution(mesh):
    cos, sin = rotary()

    def step(x, k_cache, v_cache, gain_a, wq, wo, gain_m, w_gate, w_up, w_down):
        seqs, cache = k_cache.shape[:2]
        pad = lambda t: np.concatenate([t, np.zeros(D - HEAD, np.float32)])
        small = jnp.stack([gain_a.astype(F32), gain_m.astype(F32), pad(cos), pad(sin)])
        return layer(
            x, k_cache.reshape(seqs, cache, HEAD), v_cache.reshape(seqs, cache, HEAD), small, wq, wo, w_gate, w_up, w_down
        )

    states, cache, columns, rows_of = P("dp", None), P("dp", None, "tp", None), P(None, "tp"), P("tp", None)
    return jax.shard_map(
        step,
        mesh=mesh,
        in_specs=(states, cache, cache, P(None), columns, rows_of, P(None), columns, columns, rows_of),
        out_specs=states,
        check_vma=False,
    )
```

```python
import jax
import jax.numpy as jnp
import numpy as np
from jax import lax
from jax.experimental import pallas as pl
from jax.experimental.pallas import tpu as pltpu
from jax.sharding import PartitionSpec as P

HEAD = 128
THETA = 10000
SEQS, CACHE, D, FF, TP = 64, 4096, 3072, 8192, 8
QH = 3
HALF = D // 2
HID = FF // TP
SLOTS = 6
UNIT = 2
STEPS = SEQS // (2 * UNIT)
F32, BF16 = jnp.float32, jnp.bfloat16

GROUPS = (8,) * 8
PARTS = ((0, 1, 2, 3, 4, 5), (6,), (7,))
ROWS = [sum(GROUPS[g] for g in part) for part in PARTS]
CHUNKS = 6
EXCHANGES = [(None, g, rows, 0, HALF, g < 5) for g, rows in enumerate(GROUPS)]
EXCHANGES += [(0, 0, ROWS[0], i * (HALF // CHUNKS), HALF // CHUNKS, True) for i in range(CHUNKS)]
EXCHANGES += [(1, 6, ROWS[1], 0, HALF, True), (2, 7, ROWS[2], 0, HALF, False)]
A, B, C = len(GROUPS), len(GROUPS) + CHUNKS, len(GROUPS) + CHUNKS + 1


def after():
    plan = {k: [] for k in range(STEPS)}
    late = plan[STEPS - 1]
    for g in range(5):
        for lag, what in ((0, "wo"), (1, "share"), (3, "middle"), (5, "total"), (7, "forward")):
            k = 2 * g + 1 + lag
            if k < STEPS - 1:
                plan[k].append((what, g))
            else:
                late.append((46.05, what, g))
    for k, what, g in ((11, "wo", 5), (12, "load", 0), (12, "share", 5), (13, "middle", 5), (13, "wo", 6), (14, "share", 6)):
        plan[k].append((what, g))
    late += [(44.5, "wo", 7), (45.0, "middle", 6), (45.9, "total", 5), (46.0, "share", 7), (46.1, "normed", 0), (48.35, "middle", 7)]
    late += [(t, "wide", (0, j)) for j, t in enumerate((46.2, 46.9, 47.6, 48.4))]
    for i in range(CHUNKS):
        late += [(50.8 + 0.1 * i, "share", A + i), (53.5 + 1.07 * i, "middle", A + i)]
        late += [(56.3 + 1.07 * i, "total", A + i), (59.1 + 1.07 * i, "forward", A + i), (66.0 + 0.01 * i, "out", A + i)]
    late += [(49.1 + 0.6 * i, "down", A + 2 * i) for i in range(CHUNKS // 2)]
    late += [(50.4, "total", 6), (51.4, "normed", 1), (53.6, "total", 7), (53.61, "down", B), (54.7, "normed", 2), (55.6, "share", B)]
    late += [(51.5 + 0.53 * j, "wide", (1, j)) for j in range(4)] + [(54.8 + 0.53 * j, "wide", (2, j)) for j in range(4)]
    late += [(56.9, "down", C), (58.4, "middle", B), (58.5, "share", C), (61.2, "total", B), (61.25, "middle", C), (64.0, "forward", B)]
    late += [(65.7, "total", C), (66.1, "out", B), (67.0, "out", C)]
    plan[STEPS - 1] = [entry[1:] for entry in sorted(late, key=lambda entry: entry[0])]
    return {k: entries for k, entries in plan.items() if entries}


AFTER = after()


def rotary():
    half = HEAD // 2
    angle = np.float32(CACHE - 1) * np.float32(THETA) ** (-np.arange(half, dtype=np.float32) / np.float32(half))
    cos, sin = np.cos(angle), np.sin(angle)
    rows = [np.concatenate([cos, cos]), np.concatenate([-sin, sin])]
    return np.concatenate([np.stack(rows), np.zeros((6, HEAD))]).astype(np.float32)


def kernel(
    x_hbm, k_hbm, v_hbm, gain_a_hbm, gain_m_hbm, table_hbm, wq_hbm, wo_hbm, wg_hbm, wu_hbm, wd_hbm, y_ref,
    gains, gain_rows, table, wq, wo, wg, wu, wd, kbuf, vbuf, sbuf, obuf, qbuf, xs, states, hidden, sends, gots, mines, parts, nears, lefts, rights, halves,
    ksem, vsem, wsem, widesem, downsem, xsem, ssem, rsem,
):
    me = lax.axis_index("tp")
    z, c = me // 2, me % 2
    firsts = [sum(GROUPS[:g]) for g in range(len(GROUPS))]

    barrier = pltpu.get_barrier_semaphore()
    partner = 2 * z + (1 - c)
    near, across = lax.rem(3 * z + 1, 4), 3 - z
    outer = (z == 0) | (z == 3)
    inner = (z == 1) | (z == 2)
    for peer in (partner, *[2 * lax.rem(z + d, 4) + c for d in (1, 2, 3)]):
        pl.semaphore_signal(barrier, inc=1, device_id={"tp": peer}, device_id_type=pl.DeviceIdType.MESH)

    xcopies = [
        pltpu.make_async_copy(x_hbm.at[pl.ds(firsts[g], rows), pl.ds(i * HALF, HALF)], xs[g].at[i], xsem.at[g, i])
        for g, rows in enumerate(GROUPS)
        for i in range(2)
    ]
    small_copies = [
        pltpu.make_async_copy(gain_a_hbm, gains.at[0], wsem.at[5]),
        pltpu.make_async_copy(gain_m_hbm, gains.at[1], wsem.at[6]),
        pltpu.make_async_copy(table_hbm, table, wsem.at[7]),
    ]
    wcopies = [
        pltpu.make_async_copy(source, target, wsem.at[i])
        for i, (source, target) in enumerate([(wq_hbm, wq), (wo_hbm, wo)])
    ]
    tile, chunk = 256, HALF // CHUNKS

    def columns(source, target, first, width, sem):
        at = pl.ds(first, width)
        return pltpu.make_async_copy(source.at[:, at], target.at[:, at], sem)

    wide_copies = [
        [columns(source, target, j * tile, tile, widesem.at[j, i]) for i, (source, target) in enumerate([(wg_hbm, wg), (wu_hbm, wu)])]
        for j in range(HID // tile)
    ]
    down_copies = [[columns(wd_hbm, wd, i * HALF + j * chunk, chunk, downsem.at[j, i]) for i in range(2)] for j in range(CHUNKS)]

    def kcopy(p):
        slot = lax.rem(p, SLOTS)
        return pltpu.make_async_copy(k_hbm.at[pl.ds(2 * p, 2)], kbuf.at[slot], ksem.at[slot])

    def vcopy(p):
        slot = lax.rem(p, SLOTS)
        return pltpu.make_async_copy(v_hbm.at[pl.ds(2 * p, 2)], vbuf.at[slot], vsem.at[slot])

    for copy in (*xcopies, *small_copies, wcopies[0]):
        copy.start()
    for p in range(2):
        kcopy(p).start(priority=1)
        vcopy(p).start(priority=1)

    def normed(wide, gain):
        scale = lax.rsqrt(jnp.mean(wide * wide, -1, keepdims=True) + 1e-6)
        return (wide * scale * gain).astype(BF16)

    for copy in (*xcopies, *small_copies, wcopies[0]):
        copy.wait()
    for p in range(2, SLOTS):
        kcopy(p).start(priority=1)
        vcopy(p).start(priority=1)
    wcopies[1].start(priority=1)
    for i in range(2):
        for j in range(D // HEAD):
            gain_rows[i : i + 1, j * HEAD : (j + 1) * HEAD] = gains[i].astype(F32)[j : j + 1, :]
    wide = jnp.concatenate([jnp.concatenate([x[0].astype(F32), x[1].astype(F32)], 1) for x in xs], 0)
    q = jnp.dot(normed(wide, gain_rows[0:1, :]), wq[...], preferred_element_type=F32).astype(BF16).astype(F32)
    cos, sin = table[0:1, :], table[1:2, :]
    qbuf[...] = jnp.zeros_like(qbuf)
    for s in range(QH):
        t = q[:, s * HEAD : (s + 1) * HEAD]
        turned = t * cos + pltpu.roll(t, HEAD // 2, 1) * sin
        qbuf[:, s, :] = turned.astype(BF16).astype(F32)

    def scores(p):
        slot, kept = lax.rem(p, SLOTS), lax.rem(p, 2 * UNIT)
        first = qbuf[2 * p]
        second = pltpu.roll(qbuf[2 * p + 1], QH, 0)
        row = lax.broadcasted_iota(jnp.int32, first.shape, 0)
        second = jnp.where((row >= QH) & (row < 2 * QH), second, 0.0)
        both = jnp.concatenate([first, second], 1).astype(BF16)
        for i in range(CACHE // tile):
            at = pl.ds(i * tile, tile)
            keys = jnp.concatenate([kbuf[slot, 0, at, :], kbuf[slot, 1, at, :]], 1)
            found = lax.dot_general(both, keys, (((1,), (1,)), ((), ())), preferred_element_type=F32)
            sbuf[kept, :, at] = found * HEAD**-0.5

    def finish(p):
        slot, kept = lax.rem(p, SLOTS), lax.rem(p, 2 * UNIT)
        s = sbuf[kept]
        e = jnp.exp(s - jnp.max(s, -1, keepdims=True))
        w = (e * (1.0 / jnp.sum(e, -1, keepdims=True))).astype(BF16)
        sums = [None, None]
        for i in range(CACHE // tile):
            at = pl.ds(i * tile, tile)
            values = jnp.concatenate([vbuf[slot, 0, at, :], vbuf[slot, 1, at, :]], 1)
            term = jnp.dot(w[:, i * tile : (i + 1) * tile], values, preferred_element_type=F32)
            sums[i % 2] = term if sums[i % 2] is None else sums[i % 2] + term
        for i, total in enumerate(sums):
            obuf[i, pl.ds(pl.multiple_of(16 * p, 16), 8), :] = total[:, :HEAD]
            obuf[i, pl.ds(pl.multiple_of(16 * p + 8, 8), 8), :] = pltpu.roll(total[:, HEAD:], 8 - QH, 0)

    def step(k, last):
        for u in range(UNIT):
            vcopy(k * UNIT + u).wait()
            if not last:
                kcopy((k + 1) * UNIT + u).wait()
        for u in range(UNIT):
            finish(k * UNIT + u)
        if last:
            return
        for u in range(UNIT):
            scores((k + 1) * UNIT + u)
        for u in range(UNIT):
            for copy, p in ((vcopy, k * UNIT + u), (kcopy, (k + 1) * UNIT + u)):

                @pl.when(p + SLOTS < SEQS // 2)
                def _():
                    copy(p + SLOTS).start(priority=1)

    def remote(e, i, source, target, peer):
        return pltpu.make_async_remote_copy(
            src_ref=source,
            dst_ref=target,
            send_sem=ssem.at[e, i],
            recv_sem=rsem.at[e, i],
            device_id={"tp": peer},
            device_id_type=pl.DeviceIdType.MESH,
        )

    def to_partner(e):
        return remote(e, 0, sends[e], gots[e], partner)

    def to_inner(e):
        return remote(e, 1, parts[e], nears[e], 2 * near + c)

    def two_chips(e):
        targets = [(rights, across), (rights, 3 - near), (lefts, near)]
        return [remote(e, 2 + i, parts[e], refs[e], 2 * chip + c) for i, (refs, chip) in enumerate(targets[: 1 if EXCHANGES[e][5] else 3])]

    def finished(e):
        return remote(e, 5, halves[e].at[c], halves[e].at[c], 2 * near + c)

    def halves_to_partner(e):
        return remote(e, 6, halves[e].at[c], halves[e].at[c], partner)

    def terms(exchanges, left, right_ref):
        first, columns = EXCHANGES[exchanges[0]][3:5]
        width = 512
        for mine in (False, True):
            base = (c if mine else 1 - c) * HALF + first
            for j in range(0, columns * len(exchanges), width):
                at = pl.ds(pl.multiple_of(base + j, 256), width)
                term = jnp.dot(left, right_ref[:, at], preferred_element_type=F32)
                for i in range(0, width, min(width, columns)):
                    e, to = exchanges[(j + i) // columns], (j + i) % columns
                    piece = term[:, i : i + min(width, columns)]
                    if mine:
                        mines[e][:, to : to + piece.shape[1]] = piece
                    else:
                        sends[e][:, to : to + piece.shape[1]] = piece.astype(BF16)
            if not mine:
                for e in exchanges:
                    to_partner(e).start()

    def share(e):
        to_partner(e).wait()
        total = mines[e][...] + gots[e][...].astype(F32)
        mines[e][...] = total
        parts[e][...] = total.astype(BF16)

        @pl.when(outer)
        def _():
            to_inner(e).start()

    def middle(e):
        @pl.when(inner)
        def _():
            to_inner(e).wait_recv()
            parts[e][...] = (mines[e][...] + nears[e][...].astype(F32)).astype(BF16)
            for copy in two_chips(e):
                copy.start()

    def base_of(e):
        part, g, _, first, columns, _ = EXCHANGES[e]
        if part is None:
            return xs[g][c].astype(F32)
        return jnp.concatenate([halves[g][c, :, first : first + columns].astype(F32) for g in PARTS[part]], 0)

    def total(e):
        copies = two_chips(e)

        def finish_with(ref):
            both = ref[...].astype(F32) + rights[e][...].astype(F32)
            halves[e][c] = (base_of(e) + both).astype(BF16)
            halves_to_partner(e).start()

        @pl.when(inner)
        def _():
            copies[0].wait_recv()
            finish_with(parts[e])
            if EXCHANGES[e][5]:
                finished(e).start()

        if not EXCHANGES[e][5]:

            @pl.when(outer)
            def _():
                copies[2].wait_recv()
                copies[1].wait_recv()
                finish_with(lefts[e])

    def forward(e):
        @pl.when(outer)
        def _():
            finished(e).wait_recv()
            halves_to_partner(e).start()

    def sent(e):
        @pl.when(outer)
        def _():
            to_inner(e).wait_send()

        @pl.when(inner)
        def _():
            for copy in two_chips(e):
                copy.wait_send()
            if EXCHANGES[e][5]:
                finished(e).wait_send()

    def normed_states(part):
        groups = PARTS[part]
        for g in groups:
            halves_to_partner(g).wait()
            sent(g)
        h = jnp.concatenate([jnp.concatenate([halves[g][i].astype(F32) for i in range(2)], 1) for g in groups], 0)
        states[part][...] = normed(h, gain_rows[1:2, :])

    def wide_part(part, j):
        if part == 0:
            for copy in wide_copies[j]:
                copy.wait()
        at = pl.ds(j * tile, tile)
        gate = jnp.dot(states[part][...], wg[:, at], preferred_element_type=F32)
        up = jnp.dot(states[part][...], wu[:, at], preferred_element_type=F32)
        hidden[part][:, at] = (jax.nn.silu(gate) * up).astype(BF16)

    started = set()

    def do(what, e):
        if what == "wo":
            if not started:
                pl.semaphore_wait(barrier, 4)
                wcopies[1].wait()
            started.add("wo")
            seen = []
            for s in range(QH):
                at = pl.ds(8 * firsts[e] + s, GROUPS[e], stride=8)
                seen.append(obuf[0, at, :] + obuf[1, at, :])
            terms([e], jnp.concatenate(seen, 1).astype(BF16), wo)
        elif what == "load":
            for copies in (*wide_copies, *down_copies):
                for copy in copies:
                    copy.start(priority=1)
        elif what == "share":
            share(e)
        elif what == "middle":
            middle(e)
        elif what == "total":
            total(e)
        elif what == "normed":
            normed_states(e)
        elif what == "wide":
            wide_part(*e)
        elif what == "down":
            part = EXCHANGES[e][0]
            exchanges = [e, e + 1] if part == 0 else [e]
            if part == 0:
                for i in exchanges:
                    for copy in down_copies[i - A]:
                        copy.wait()
            terms(exchanges, hidden[part][...], wd)
        elif what == "forward":
            forward(e)
        elif what == "out":
            halves_to_partner(e).wait()
            sent(e)
            _, g, rows, first, columns, _ = EXCHANGES[e]
            for i in range(2):
                y_ref[firsts[g] : firsts[g] + rows, i * HALF + first : i * HALF + first + columns] = halves[e][i]

    for u in range(UNIT):
        kcopy(u).wait()
        scores(u)
        kcopy(u + SLOTS).start(priority=1)
    at = 0
    for k in sorted(AFTER):
        if k < STEPS - 1:
            lax.fori_loop(at, k + 1, lambda i, _: step(i, False), None)
        else:
            if at < STEPS - 1:
                lax.fori_loop(at, STEPS - 1, lambda i, _: step(i, False), None)
            step(STEPS - 1, True)
        at = k + 1
        for what, e in AFTER[k]:
            do(what, e)


def layer(x, k, v, gain_a, gain_m, table, wq, wo, wg, wu, wd):
    n = len(EXCHANGES)
    each = lambda *lead, dtype=BF16: [pltpu.VMEM((*lead, rows, width), dtype) for _, _, rows, _, width, _ in EXCHANGES]
    parts = lambda width: [pltpu.VMEM((rows, width), BF16) for rows in ROWS]
    return pl.pallas_call(
        kernel,
        out_shape=jax.ShapeDtypeStruct((SEQS, D), BF16),
        in_specs=[pl.BlockSpec(memory_space=pltpu.HBM)] * 11,
        out_specs=pl.BlockSpec(memory_space=pltpu.VMEM),
        scratch_shapes=[
            pltpu.VMEM((2, *gain_a.shape), BF16),
            pltpu.VMEM((2, D), F32),
            pltpu.VMEM(table.shape, F32),
            pltpu.VMEM(wq.shape, BF16),
            pltpu.VMEM(wo.shape, BF16),
            pltpu.VMEM(wg.shape, BF16),
            pltpu.VMEM(wu.shape, BF16),
            pltpu.VMEM(wd.shape, BF16),
            pltpu.VMEM((SLOTS, 2, CACHE, HEAD), BF16),
            pltpu.VMEM((SLOTS, 2, CACHE, HEAD), BF16),
            pltpu.VMEM((2 * UNIT, 8, CACHE), F32),
            pltpu.VMEM((2, SEQS * 8, HEAD), F32),
            pltpu.VMEM((SEQS, 8, HEAD), F32),
            [pltpu.VMEM((2, rows, HALF), BF16) for rows in GROUPS],
            parts(D),
            parts(HID),
            each(),
            each(),
            each(dtype=F32),
            each(),
            each(),
            each(),
            each(),
            each(2),
            pltpu.SemaphoreType.DMA((SLOTS,)),
            pltpu.SemaphoreType.DMA((SLOTS,)),
            pltpu.SemaphoreType.DMA((8,)),
            pltpu.SemaphoreType.DMA((HID // 256, 2)),
            pltpu.SemaphoreType.DMA((CHUNKS, 2)),
            pltpu.SemaphoreType.DMA((len(GROUPS), 2)),
            pltpu.SemaphoreType.DMA((n, 7)),
            pltpu.SemaphoreType.DMA((n, 7)),
        ],
        compiler_params=pltpu.CompilerParams(collective_id=0, has_side_effects=True, vmem_limit_bytes=63 * 2**20),
    )(x, k, v, gain_a, gain_m, table, wq, wo, wg, wu, wd)


def solution(mesh):
    table = rotary()

    def step(x, k_cache, v_cache, gain_a, wq, wo, gain_m, w_gate, w_up, w_down):
        seqs, cache = k_cache.shape[:2]
        k, v = (t.reshape(seqs, cache, HEAD) for t in (k_cache, v_cache))
        gain_a, gain_m = (t.reshape(-1, HEAD) for t in (gain_a, gain_m))
        return layer(x, k, v, gain_a, gain_m, jnp.asarray(table), wq, wo, w_gate, w_up, w_down)

    states, cache, columns, rows_of = P("dp", None), P("dp", None, "tp", None), P(None, "tp"), P("tp", None)
    return jax.shard_map(
        step,
        mesh=mesh,
        in_specs=(states, cache, cache, P(None), columns, rows_of, P(None), columns, columns, rows_of),
        out_specs=states,
        check_vma=False,
    )
```

```python
import jax
import jax.numpy as jnp
import numpy as np
from jax import lax
from jax.experimental import pallas as pl
from jax.experimental.pallas import tpu as pltpu
from jax.sharding import PartitionSpec as P

HEAD = 128
THETA = 10000
SEQS, CACHE, D, FF, TP = 64, 4096, 3072, 8192, 8
QH = 3
HALF = D // 2
HID = FF // TP
SLOTS = 6
UNIT = 2
STEPS = SEQS // (2 * UNIT)
F32, BF16 = jnp.float32, jnp.bfloat16

GROUPS = (8,) * 8
PARTS = ((0, 1, 2, 3, 4, 5), (6,), (7,))
ROWS = [sum(GROUPS[g] for g in part) for part in PARTS]
CHUNKS = 6
EXCHANGES = [(None, g, rows, 0, HALF, g < 5) for g, rows in enumerate(GROUPS)]
EXCHANGES += [(0, 0, ROWS[0], i * (HALF // CHUNKS), HALF // CHUNKS, True) for i in range(CHUNKS)]
EXCHANGES += [(1, 6, ROWS[1], 0, HALF, True), (2, 7, ROWS[2], 0, HALF, False)]
A, B, C = len(GROUPS), len(GROUPS) + CHUNKS, len(GROUPS) + CHUNKS + 1


def after():
    plan = {k: [] for k in range(STEPS)}
    late = plan[STEPS - 1]
    for g in range(5):
        for lag, what in ((0, "wo"), (1, "share"), (3, "middle"), (5, "total"), (7, "forward")):
            k = 2 * g + 1 + lag
            if k < STEPS - 1:
                plan[k].append((what, g))
            else:
                late.append((46.05, what, g))
    for k, what, g in ((11, "wo", 5), (12, "load", 0), (12, "share", 5), (13, "middle", 5), (13, "wo", 6), (14, "share", 6)):
        plan[k].append((what, g))
    late += [(44.5, "wo", 7), (45.0, "middle", 6), (45.9, "total", 5), (46.0, "share", 7), (46.1, "normed", 0), (48.35, "middle", 7)]
    late += [(t, "wide", (0, j)) for j, t in enumerate((46.2, 46.9, 47.6, 48.4))]
    for i in range(CHUNKS):
        late += [((50.8 if i < 4 else 51.6) + 0.1 * i, "share", A + i), ((53.5 + 1.07 * i) if i < 4 else 57.0 + 0.01 * i, "middle", A + i)]
        late += [(57.2 + 0.05 * i, "total", A + i), (59.1 + 1.07 * i, "forward", A + i), (66.0 + 0.01 * i, "out", A + i)]
    late += [(49.1 + 0.6 * i, "down", A + 2 * i) for i in range(CHUNKS // 2)]
    late += [(50.4, "total", 6), (51.4, "normed", 1), (53.6, "total", 7), (53.61, "down", B), (54.7, "normed", 2), (55.6, "share", B)]
    late += [(51.5 + 1.06 * j, "wide", (1, j)) for j in range(2)] + [(54.8 + 1.06 * j, "wide", (2, j)) for j in range(2)]
    late += [(56.9, "down", C), (57.0, "share", C), (57.15, "middle", B), (57.36, "middle", C), (57.42, "total", B), (64.0, "forward", B)]
    late += [(65.7, "total", C), (66.1, "out", B), (67.0, "out", C)]
    plan[STEPS - 1] = [entry[1:] for entry in sorted(late, key=lambda entry: entry[0])]
    return {k: entries for k, entries in plan.items() if entries}


AFTER = after()


def rotary():
    half = HEAD // 2
    angle = np.float32(CACHE - 1) * np.float32(THETA) ** (-np.arange(half, dtype=np.float32) / np.float32(half))
    cos, sin = np.cos(angle), np.sin(angle)
    rows = [np.concatenate([cos, cos]), np.concatenate([-sin, sin])]
    return np.concatenate([np.stack(rows), np.zeros((6, HEAD))]).astype(np.float32)


def kernel(
    x_hbm, k_hbm, v_hbm, gain_a_hbm, gain_m_hbm, table_hbm, wq_hbm, wo_hbm, wg_hbm, wu_hbm, wd_hbm, y_hbm,
    gains, gain_rows, table, wq, wo, wg, wu, wd, kbuf, vbuf, sbuf, obuf, qbuf, xs, states, hidden, sends, gots, mines, parts, nears, lefts, rights, halves,
    ksem, vsem, wsem, widesem, downsem, xsem, ysem, ssem, rsem,
):
    me = lax.axis_index("tp")
    z, c = me // 2, me % 2
    firsts = [sum(GROUPS[:g]) for g in range(len(GROUPS))]

    barrier = pltpu.get_barrier_semaphore()
    partner = 2 * z + (1 - c)
    near, across = lax.rem(3 * z + 1, 4), 3 - z
    outer = (z == 0) | (z == 3)
    inner = (z == 1) | (z == 2)
    for peer in (partner, *[2 * lax.rem(z + d, 4) + c for d in (1, 2, 3)]):
        pl.semaphore_signal(barrier, inc=1, device_id={"tp": peer}, device_id_type=pl.DeviceIdType.MESH)

    xcopies = [
        pltpu.make_async_copy(x_hbm.at[pl.ds(firsts[g], rows), pl.ds(i * HALF, HALF)], xs[g].at[i], xsem.at[g, i])
        for g, rows in enumerate(GROUPS)
        for i in range(2)
    ]
    small_copies = [
        pltpu.make_async_copy(gain_a_hbm, gains.at[0], wsem.at[5]),
        pltpu.make_async_copy(gain_m_hbm, gains.at[1], wsem.at[6]),
        pltpu.make_async_copy(table_hbm, table, wsem.at[7]),
    ]
    wcopies = [
        pltpu.make_async_copy(source, target, wsem.at[i])
        for i, (source, target) in enumerate([(wq_hbm, wq), (wo_hbm, wo)])
    ]
    tile, chunk = 256, HALF // CHUNKS

    def columns(source, target, first, width, sem):
        at = pl.ds(first, width)
        return pltpu.make_async_copy(source.at[:, at], target.at[:, at], sem)

    wide_copies = [
        [columns(source, target, j * tile, tile, widesem.at[j, i]) for i, (source, target) in enumerate([(wg_hbm, wg), (wu_hbm, wu)])]
        for j in range(HID // tile)
    ]
    down_copies = [[columns(wd_hbm, wd, i * HALF + j * chunk, chunk, downsem.at[j, i]) for i in range(2)] for j in range(CHUNKS)]

    def kcopy(p):
        slot = lax.rem(p, SLOTS)
        return pltpu.make_async_copy(k_hbm.at[pl.ds(2 * p, 2)], kbuf.at[slot], ksem.at[slot])

    def vcopy(p):
        slot = lax.rem(p, SLOTS)
        return pltpu.make_async_copy(v_hbm.at[pl.ds(2 * p, 2)], vbuf.at[slot], vsem.at[slot])

    for copy in (*xcopies, *small_copies, wcopies[0]):
        copy.start()
    for p in range(2):
        kcopy(p).start(priority=1)
        vcopy(p).start(priority=1)

    def normed(wide, gain):
        scale = lax.rsqrt(jnp.mean(wide * wide, -1, keepdims=True) + 1e-6)
        return (wide * scale * gain).astype(BF16)

    for copy in (*xcopies, *small_copies, wcopies[0]):
        copy.wait()
    for p in range(2, SLOTS):
        kcopy(p).start(priority=1)
        vcopy(p).start(priority=1)
    wcopies[1].start(priority=1)
    for i in range(2):
        for j in range(D // HEAD):
            gain_rows[i : i + 1, j * HEAD : (j + 1) * HEAD] = gains[i].astype(F32)[j : j + 1, :]
    wide = jnp.concatenate([jnp.concatenate([x[0].astype(F32), x[1].astype(F32)], 1) for x in xs], 0)
    q = jnp.dot(normed(wide, gain_rows[0:1, :]), wq[...], preferred_element_type=F32).astype(BF16).astype(F32)
    cos, sin = table[0:1, :], table[1:2, :]
    qbuf[...] = jnp.zeros_like(qbuf)
    for s in range(QH):
        t = q[:, s * HEAD : (s + 1) * HEAD]
        turned = t * cos + pltpu.roll(t, HEAD // 2, 1) * sin
        qbuf[:, s, :] = turned.astype(BF16).astype(F32)

    def scores(p):
        slot, kept = lax.rem(p, SLOTS), lax.rem(p, 2 * UNIT)
        first = qbuf[2 * p]
        second = pltpu.roll(qbuf[2 * p + 1], QH, 0)
        row = lax.broadcasted_iota(jnp.int32, first.shape, 0)
        second = jnp.where((row >= QH) & (row < 2 * QH), second, 0.0)
        both = jnp.concatenate([first, second], 1).astype(BF16)
        for i in range(CACHE // tile):
            at = pl.ds(i * tile, tile)
            keys = jnp.concatenate([kbuf[slot, 0, at, :], kbuf[slot, 1, at, :]], 1)
            found = lax.dot_general(both, keys, (((1,), (1,)), ((), ())), preferred_element_type=F32)
            sbuf[kept, :, at] = found * HEAD**-0.5

    def finish(p):
        slot, kept = lax.rem(p, SLOTS), lax.rem(p, 2 * UNIT)
        s = sbuf[kept]
        e = jnp.exp(s - jnp.max(s, -1, keepdims=True))
        w = (e * (1.0 / jnp.sum(e, -1, keepdims=True))).astype(BF16)
        sums = [None, None]
        for i in range(CACHE // tile):
            at = pl.ds(i * tile, tile)
            values = jnp.concatenate([vbuf[slot, 0, at, :], vbuf[slot, 1, at, :]], 1)
            term = jnp.dot(w[:, i * tile : (i + 1) * tile], values, preferred_element_type=F32)
            sums[i % 2] = term if sums[i % 2] is None else sums[i % 2] + term
        for i, total in enumerate(sums):
            obuf[i, pl.ds(pl.multiple_of(16 * p, 16), 8), :] = total[:, :HEAD]
            obuf[i, pl.ds(pl.multiple_of(16 * p + 8, 8), 8), :] = pltpu.roll(total[:, HEAD:], 8 - QH, 0)

    def step(k, last):
        for u in range(UNIT):
            vcopy(k * UNIT + u).wait()
            if not last:
                kcopy((k + 1) * UNIT + u).wait()
        for u in range(UNIT):
            finish(k * UNIT + u)
        if last:
            return
        for u in range(UNIT):
            scores((k + 1) * UNIT + u)
        for u in range(UNIT):
            for copy, p in ((vcopy, k * UNIT + u), (kcopy, (k + 1) * UNIT + u)):

                @pl.when(p + SLOTS < SEQS // 2)
                def _():
                    copy(p + SLOTS).start(priority=1)

    def remote(e, i, source, target, peer):
        return pltpu.make_async_remote_copy(
            src_ref=source,
            dst_ref=target,
            send_sem=ssem.at[e, i],
            recv_sem=rsem.at[e, i],
            device_id={"tp": peer},
            device_id_type=pl.DeviceIdType.MESH,
        )

    def to_partner(e):
        return remote(e, 0, sends[e], gots[e], partner)

    def to_inner(e):
        return remote(e, 1, parts[e], nears[e], 2 * near + c)

    def two_chips(e):
        targets = [(rights, across), (rights, 3 - near), (lefts, near)]
        return [remote(e, 2 + i, parts[e], refs[e], 2 * chip + c) for i, (refs, chip) in enumerate(targets[: 1 if EXCHANGES[e][5] else 3])]

    def finished(e):
        return remote(e, 5, halves[e].at[c], halves[e].at[c], 2 * near + c)

    def halves_to_partner(e):
        return remote(e, 6, halves[e].at[c], halves[e].at[c], partner)

    def terms(exchanges, left, right_ref):
        first, columns = EXCHANGES[exchanges[0]][3:5]
        width = 512
        for mine in (False, True):
            base = (c if mine else 1 - c) * HALF + first
            for j in range(0, columns * len(exchanges), width):
                at = pl.ds(pl.multiple_of(base + j, 256), width)
                term = jnp.dot(left, right_ref[:, at], preferred_element_type=F32)
                for i in range(0, width, min(width, columns)):
                    e, to = exchanges[(j + i) // columns], (j + i) % columns
                    piece = term[:, i : i + min(width, columns)]
                    if mine:
                        mines[e][:, to : to + piece.shape[1]] = piece
                    else:
                        sends[e][:, to : to + piece.shape[1]] = piece.astype(BF16)
            if not mine:
                for e in exchanges:
                    to_partner(e).start()

    def share(e):
        to_partner(e).wait()
        total = mines[e][...] + gots[e][...].astype(F32)
        mines[e][...] = total
        parts[e][...] = total.astype(BF16)

        @pl.when(outer)
        def _():
            to_inner(e).start()

    def middle(e):
        @pl.when(inner)
        def _():
            to_inner(e).wait_recv()
            parts[e][...] = (mines[e][...] + nears[e][...].astype(F32)).astype(BF16)
            for copy in two_chips(e):
                copy.start()

    def base_of(e):
        part, g, _, first, columns, _ = EXCHANGES[e]
        if part is None:
            return xs[g][c].astype(F32)
        return jnp.concatenate([halves[g][c, :, first : first + columns].astype(F32) for g in PARTS[part]], 0)

    def total(e):
        copies = two_chips(e)

        def finish_with(ref):
            both = ref[...].astype(F32) + rights[e][...].astype(F32)
            halves[e][c] = (base_of(e) + both).astype(BF16)
            halves_to_partner(e).start()

        @pl.when(inner)
        def _():
            copies[0].wait_recv()
            finish_with(parts[e])
            if EXCHANGES[e][5]:
                finished(e).start()

        if not EXCHANGES[e][5]:

            @pl.when(outer)
            def _():
                copies[2].wait_recv()
                copies[1].wait_recv()
                finish_with(lefts[e])

    def forward(e):
        @pl.when(outer)
        def _():
            finished(e).wait_recv()
            halves_to_partner(e).start()

    def sent(e):
        @pl.when(outer)
        def _():
            to_inner(e).wait_send()

        @pl.when(inner)
        def _():
            for copy in two_chips(e):
                copy.wait_send()
            if EXCHANGES[e][5]:
                finished(e).wait_send()

    def normed_states(part):
        groups = PARTS[part]
        for g in groups:
            halves_to_partner(g).wait()
            sent(g)
        h = jnp.concatenate([jnp.concatenate([halves[g][i].astype(F32) for i in range(2)], 1) for g in groups], 0)
        states[part][...] = normed(h, gain_rows[1:2, :])

    def wide_part(part, j):
        if part == 0:
            for copy in wide_copies[j]:
                copy.wait()
        width = tile if part == 0 else HID // 2
        at = pl.ds(j * width, width)
        gate = jnp.dot(states[part][...], wg[:, at], preferred_element_type=F32)
        up = jnp.dot(states[part][...], wu[:, at], preferred_element_type=F32)
        hidden[part][:, at] = (jax.nn.silu(gate) * up).astype(BF16)

    started = set()

    def do(what, e):
        if what == "wo":
            if not started:
                pl.semaphore_wait(barrier, 4)
                wcopies[1].wait()
            started.add("wo")
            seen = []
            for s in range(QH):
                at = pl.ds(8 * firsts[e] + s, GROUPS[e], stride=8)
                seen.append(obuf[0, at, :] + obuf[1, at, :])
            terms([e], jnp.concatenate(seen, 1).astype(BF16), wo)
        elif what == "load":
            for copies in (*wide_copies, *down_copies):
                for copy in copies:
                    copy.start(priority=1)
        elif what == "share":
            share(e)
        elif what == "middle":
            middle(e)
        elif what == "total":
            total(e)
        elif what == "normed":
            normed_states(e)
        elif what == "wide":
            wide_part(*e)
        elif what == "down":
            part = EXCHANGES[e][0]
            exchanges = [e, e + 1] if part == 0 else [e]
            if part == 0:
                for i in exchanges:
                    for copy in down_copies[i - A]:
                        copy.wait()
            terms(exchanges, hidden[part][...], wd)
        elif what == "forward":
            forward(e)
        elif what == "out":
            halves_to_partner(e).wait()
            sent(e)
            for copy in ycopies(e):
                copy.start()

    def ycopies(e):
        _, g, rows, first, columns, _ = EXCHANGES[e]
        return [
            pltpu.make_async_copy(
                halves[e].at[i], y_hbm.at[pl.ds(firsts[g], rows), pl.ds(i * HALF + first, columns)], ysem.at[e - A, i]
            )
            for i in range(2)
        ]

    for u in range(UNIT):
        kcopy(u).wait()
        scores(u)
        kcopy(u + SLOTS).start(priority=1)
    at = 0
    for k in sorted(AFTER):
        if k < STEPS - 1:
            lax.fori_loop(at, k + 1, lambda i, _: step(i, False), None)
        else:
            if at < STEPS - 1:
                lax.fori_loop(at, STEPS - 1, lambda i, _: step(i, False), None)
            step(STEPS - 1, True)
        at = k + 1
        for what, e in AFTER[k]:
            do(what, e)
    for e in range(A, len(EXCHANGES)):
        for copy in ycopies(e):
            copy.wait()


def layer(x, k, v, gain_a, gain_m, table, wq, wo, wg, wu, wd):
    n = len(EXCHANGES)
    each = lambda *lead, dtype=BF16: [pltpu.VMEM((*lead, rows, width), dtype) for _, _, rows, _, width, _ in EXCHANGES]
    parts = lambda width: [pltpu.VMEM((rows, width), BF16) for rows in ROWS]
    return pl.pallas_call(
        kernel,
        out_shape=jax.ShapeDtypeStruct((SEQS, D), BF16),
        in_specs=[pl.BlockSpec(memory_space=pltpu.HBM)] * 11,
        out_specs=pl.BlockSpec(memory_space=pltpu.HBM),
        scratch_shapes=[
            pltpu.VMEM((2, *gain_a.shape), BF16),
            pltpu.VMEM((2, D), F32),
            pltpu.VMEM(table.shape, F32),
            pltpu.VMEM(wq.shape, BF16),
            pltpu.VMEM(wo.shape, BF16),
            pltpu.VMEM(wg.shape, BF16),
            pltpu.VMEM(wu.shape, BF16),
            pltpu.VMEM(wd.shape, BF16),
            pltpu.VMEM((SLOTS, 2, CACHE, HEAD), BF16),
            pltpu.VMEM((SLOTS, 2, CACHE, HEAD), BF16),
            pltpu.VMEM((2 * UNIT, 8, CACHE), F32),
            pltpu.VMEM((2, SEQS * 8, HEAD), F32),
            pltpu.VMEM((SEQS, 8, HEAD), F32),
            [pltpu.VMEM((2, rows, HALF), BF16) for rows in GROUPS],
            parts(D),
            parts(HID),
            each(),
            each(),
            each(dtype=F32),
            each(),
            each(),
            each(),
            each(),
            each(2),
            pltpu.SemaphoreType.DMA((SLOTS,)),
            pltpu.SemaphoreType.DMA((SLOTS,)),
            pltpu.SemaphoreType.DMA((8,)),
            pltpu.SemaphoreType.DMA((HID // 256, 2)),
            pltpu.SemaphoreType.DMA((CHUNKS, 2)),
            pltpu.SemaphoreType.DMA((len(GROUPS), 2)),
            pltpu.SemaphoreType.DMA((n - A, 2)),
            pltpu.SemaphoreType.DMA((n, 7)),
            pltpu.SemaphoreType.DMA((n, 7)),
        ],
        compiler_params=pltpu.CompilerParams(collective_id=0, has_side_effects=True, vmem_limit_bytes=63 * 2**20),
    )(x, k, v, gain_a, gain_m, table, wq, wo, wg, wu, wd)


def solution(mesh):
    table = rotary()

    def step(x, k_cache, v_cache, gain_a, wq, wo, gain_m, w_gate, w_up, w_down):
        seqs, cache = k_cache.shape[:2]
        k, v = (t.reshape(seqs, cache, HEAD) for t in (k_cache, v_cache))
        gain_a, gain_m = (t.reshape(-1, HEAD) for t in (gain_a, gain_m))
        return layer(x, k, v, gain_a, gain_m, jnp.asarray(table), wq, wo, w_gate, w_up, w_down)

    states, cache, columns, rows_of = P("dp", None), P("dp", None, "tp", None), P(None, "tp"), P("tp", None)
    return jax.shard_map(
        step,
        mesh=mesh,
        in_specs=(states, cache, cache, P(None), columns, rows_of, P(None), columns, columns, rows_of),
        out_specs=states,
        check_vma=False,
    )
```
